32 devices in a mesh: dp: 2 (over core), fsdp: 16 (over z, y, x).
Axes of the slice: x: 2, y: 2, z: 4, core: 2. Of those that a mesh axis runs over, the one named last changes fastest.
Arguments:
- tokens: bfloat16 [8192, 4096], P(('dp', 'fsdp')), may hold values from -6 to 6
- block_codes: bfloat16 [256, 128, 128], P('fsdp'), may hold values from -4 to 4
- scales: float32 [256], P('fsdp'), may hold values from 0.008 to 0.03
- counts: int32 [16], replicated, may hold values from 0 to 16, as said below
- cotangent: bfloat16 [8192, 512], P(('dp', 'fsdp')), may hold values from -6 to 6
Outputs:
- projected: bfloat16 [8192, 512], P(('dp', 'fsdp'))
- token_grad: bfloat16 [8192, 4096], P(('dp', 'fsdp'))
- block_grad: bfloat16 [256, 128, 128], P('fsdp')
The draws below stay inside these ranges and needn't reach their ends.
Inputs may be any that keep to these rules, and one draw needn't show every extreme that they name: counts sum to 128; each is at most 16, and some owner has exactly 16 and some none; slots past an owner's count hold values that are not used.
All inputs are finite; a program needn't handle non-finite values.
Results may differ from the reference program's by a relative error of at most 0.009.
Values may be sent and summed in bfloat16 or wider, within the bound.
A program may use at most 128 MiB of HBM per device.

```python
import math
import jax
import jax.numpy as jnp
from jax import lax

D = 4096
KC = 512
TILE = 128
TOKENS = 8192
NBLK = 128
MEAN = 8
MOST = 16
N_FSDP = 16


def draw_counts(key, part):
    shuffled = jax.random.permutation(jax.random.fold_in(key, 11), N_FSDP)
    amounts = jax.random.randint(jax.random.fold_in(key, 12), (N_FSDP // 2,), 0, MEAN + 1)
    amounts = amounts.at[0].set(MEAN)
    shifts = jnp.zeros((N_FSDP,), jnp.int32)
    shifts = shifts.at[shuffled[0::2]].set(amounts).at[shuffled[1::2]].set(-amounts)
    return (MEAN + shifts).astype(jnp.int32)


def strengthened(values, own_key, source, target, blocks, factor):
    owner, partner = [(jnp.arange(values.shape[dim]) // (values.shape[dim] // blocks)).reshape([-1 if axis == dim else 1 for axis in range(values.ndim)]) for dim in (source, target)]
    chosen = jax.random.permutation(own_key, blocks)[partner]
    strong = (owner == chosen) | (owner == (partner + blocks // 2) % blocks)
    return jnp.where(strong, factor * values, values)


def steps_of(own_key, shape, split, low, high):
    loudness = 1.0
    for dim, parts in split:
        steps = jax.random.uniform(jax.random.fold_in(jax.random.fold_in(own_key, 6), dim), (parts,), jnp.float32, low / len(split), high / len(split))
        loudness = loudness * jnp.repeat(jnp.exp(steps), shape[dim] // parts).reshape((-1,) + (1,) * (len(shape) - 1 - dim))
    return loudness


def normal_values(own_key, shape, scale, most, cuts=(), held_as=jnp.bfloat16):
    loudness = steps_of(own_key, shape, cuts, -0.22, 0.18) if cuts else 1.0
    values = jax.random.normal(own_key, shape, jnp.float32) * scale * loudness
    return jnp.minimum(jnp.maximum(values, -most), most).astype(held_as)


def heavy_noise(stream_key, extent, width, limit, cuts, heavy, kind=jnp.bfloat16):
    values = width * jax.random.normal(stream_key, extent, jnp.float32)
    if cuts:
        values = values * steps_of(stream_key, extent, cuts, -0.22, 0.18)
    return jnp.clip(strengthened(values, jax.random.fold_in(stream_key, 3), *heavy), -limit, limit).astype(kind)


def setup_inputs(seed: int = 0) -> dict:
    arg_keys = jax.random.split(jax.random.key(seed), 6)
    tokens = heavy_noise(arg_keys[0], (TOKENS, D), 1.0, 6.0, ((0, 32),), (0, 1, 32, 2.75))
    block_codes = normal_values(arg_keys[1], (N_FSDP * MOST, TILE, TILE), 1.0, 4.0, ((0, 16),))
    scales = jnp.clip(jnp.exp(math.log(0.03) - 1.3217558 * jax.random.uniform(arg_keys[2], (N_FSDP * MOST,), jnp.float32) ** steps_of(arg_keys[2], (N_FSDP * MOST,), ((0, 16),), -0.2, 0.2)), 0.008, 0.03)
    counts = draw_counts(jax.random.fold_in(arg_keys[5], 71), 0)
    cotangent = normal_values(arg_keys[4], (TOKENS, KC), 1.0, 6.0, ((0, 32),))
    return {"tokens": tokens, "block_codes": block_codes, "scales": scales, "counts": counts, "cotangent": cotangent}


def block_index(counts):
    run_ends = jnp.cumsum(counts).astype(jnp.int32)
    offsets = (run_ends - counts).astype(jnp.int32)
    block_ids = jnp.arange(NBLK, dtype=jnp.int32)
    owners = lax.optimization_barrier(jnp.sum((run_ends[None, :] <= block_ids[:, None]).astype(jnp.int32), axis=1))
    matched = owners[:, None] == jnp.arange(N_FSDP, dtype=jnp.int32)[None, :]
    run_start = lax.optimization_barrier(jnp.sum(jnp.where(matched, offsets[None, :], 0), axis=1)).astype(jnp.int32)
    source_ids = (owners * MOST + block_ids - run_start).astype(jnp.int32)
    return (offsets, source_ids)

def reference(tokens, block_codes, scales, counts, cotangent):
    offsets, source_ids = block_index(counts)
    blocks = block_codes[source_ids].astype(jnp.float32) * scales[source_ids][:, None, None]
    blocks = blocks.astype(jnp.bfloat16)
    weight = blocks.reshape(D // TILE, KC // TILE, TILE, TILE).transpose(0, 2, 1, 3).reshape(D, KC)
    projected = jnp.dot(tokens, weight, preferred_element_type=jnp.float32).astype(jnp.bfloat16)
    token_grad = jnp.dot(cotangent, weight.T, preferred_element_type=jnp.float32).astype(jnp.bfloat16)
    grad = jnp.dot(tokens.T, cotangent, preferred_element_type=jnp.float32) * (1.0 / math.sqrt(TOKENS))
    grad_blocks = grad.reshape(D // TILE, TILE, KC // TILE, TILE).transpose(0, 2, 1, 3).reshape(NBLK, TILE, TILE)
    slot_ids = jnp.arange(N_FSDP * MOST, dtype=jnp.int32)
    owner_of = slot_ids // MOST
    within = slot_ids % MOST
    wanted = (offsets[owner_of] + within).astype(jnp.int32)
    is_valid = within < counts[owner_of]
    picked = grad_blocks[jnp.clip(wanted, 0, NBLK - 1)]
    block_grad = jnp.where(is_valid[:, None, None], picked, jnp.float32(0.0)).astype(jnp.bfloat16)
    return (projected, token_grad, block_grad)
```

```python
import functools
import math

import jax
import jax.numpy as jnp
from jax import lax
from jax.experimental import pallas as pl
from jax.experimental.pallas import tpu as pltpu
from jax.sharding import PartitionSpec as P

MESH = pl.DeviceIdType.MESH
F32 = jnp.float32
BF16 = jnp.bfloat16


def block_index(counts, owners_total, block_count, most_slots):
    run_ends = jnp.cumsum(counts)
    offsets = run_ends - counts
    block_ids = jnp.arange(block_count, dtype=jnp.int32)
    owners = jnp.sum((run_ends[None, :] <= block_ids[:, None]).astype(jnp.int32), axis=1)
    matched = owners[:, None] == jnp.arange(owners_total, dtype=jnp.int32)[None, :]
    run_start = jnp.sum(jnp.where(matched, offsets[None, :], 0), axis=1)
    source_ids = owners * most_slots + block_ids - run_start
    return (offsets, source_ids)


def grad_kernel(scale, tile, tok_ref, cot_ref, out_ref):
    half = tile // 2
    part = lax.dot_general(
        tok_ref[...], cot_ref[...], (((0,), (0,)), ((), ())), preferred_element_type=F32
    )
    part = (part * scale).astype(BF16)
    rows, cols = part.shape[0] // tile, part.shape[1] // tile
    for r in range(rows):
        for c in range(cols):
            for h in range(2):
                top = r * tile + h * half
                out_ref[h, r * cols + c] = part[top : top + half, c * tile : (c + 1) * tile]


def weight_kernel(tile, chunks, ids_ref, tok_ref, cot_ref, held_ref, proj_ref, tg_ref, w_ref, acc_ref, sems):
    step = pl.program_id(0)
    depth = w_ref.shape[1]
    cols = w_ref.shape[2] // tile
    rows = depth // tile

    @pl.when(step == 0)
    def _():
        def fetch(g, _):
            for r in range(rows):
                for c in range(cols):
                    b = (g * rows + r) * cols + c
                    pltpu.make_async_copy(
                        held_ref.at[ids_ref[b]],
                        w_ref.at[g, pl.ds(r * tile, tile), pl.ds(c * tile, tile)],
                        sems.at[g],
                    ).start()
            return 0

        lax.fori_loop(0, chunks, fetch, 0)
        acc_ref[...] = jnp.zeros_like(acc_ref)

    pltpu.make_async_copy(w_ref.at[step], w_ref.at[step], sems.at[step]).wait()
    weight = w_ref[step]
    acc_ref[...] += jnp.dot(tok_ref[...], weight, preferred_element_type=F32)
    tg_ref[...] = lax.dot_general(
        cot_ref[...], weight, (((1,), (1,)), ((), ())), preferred_element_type=F32
    ).astype(BF16)

    @pl.when(step == chunks - 1)
    def _():
        proj_ref[...] = acc_ref[...].astype(BF16)


def comm_kernel(
    outer, inner, idx_ref, own_ref, g_ref, held_ref, out_ref,
    pair_buf, sb, ra1, rb1, ta, tb, ra2, rb2,
    local_sem, pair_sems, gi_send, gi_recv, go_send, go_recv, fi_send, fi_recv, fo_send, fo_recv,
    ri_send, ri_recv, ro_send, ro_recv, out_sems,
):
    core = lax.axis_index("dp")
    other = 1 - core
    me = lax.axis_index("fsdp")
    o = me // inner
    i = me % inner
    slots, tile = own_ref.shape[0], own_ref.shape[1]
    half, q = tile // 2, tile // 4

    def rows(c, p):
        return pl.ds(pl.multiple_of(c * half + p * q, q), q)

    partner = (other, me)

    def mate_in(k):
        return (core, o * inner + (i + k) % inner)

    def mate_out(k):
        return (core, ((o + k) % outer) * inner + i)

    def remote(src, dst, send, recv, device):
        return pltpu.make_async_remote_copy(
            src_ref=src, dst_ref=dst, send_sem=send, recv_sem=recv,
            device_id=device, device_id_type=MESH,
        )

    barrier = pltpu.get_barrier_semaphore()
    peers = [partner] + [mate_in(k) for k in range(1, inner)] + [mate_out(k) for k in range(1, outer)]
    for peer in peers:
        pl.semaphore_signal(barrier, inc=1, device_id=peer, device_id_type=MESH)
    pl.semaphore_wait(barrier, len(peers))

    started = []

    def go(copy):
        copy.start()
        started.append(copy)
        return copy

    pair = remote(g_ref.at[other], pair_buf, pair_sems.at[0], pair_sems.at[1], partner)
    pair.start()
    a1 = [
        go(remote(own_ref.at[:, rows(core, 0)], held_ref.at[o, i, :, rows(core, 0)],
                  gi_send.at[0, k], gi_recv.at[0, k], mate_in(k)))
        for k in range(1, inner)
    ]
    b1 = [
        go(remote(own_ref.at[:, rows(core, 1)], held_ref.at[o, i, :, rows(core, 1)],
                  go_send.at[0, k], go_recv.at[0, k], mate_out(k)))
        for k in range(1, outer)
    ]
    mine = pltpu.make_async_copy(own_ref, held_ref.at[o, i], local_sem)
    mine.start()

    pair.wait_recv()

    def build(s, _):
        oo, ii, j = s // (inner * slots), (s // slots) % inner, s % slots
        b = idx_ref[s]
        total = g_ref[core, b].astype(F32) + pair_buf[b].astype(F32)
        total = total.astype(BF16)
        sb[0, oo, ii, j] = total[:q]
        sb[1, oo, ii, j] = total[q:]
        return 0

    lax.fori_loop(0, outer * inner * slots, build, 0, unroll=4)

    ga1 = [
        go(remote(sb.at[0, (o + k) % outer], ra1.at[k], ro_send.at[0, k], ro_recv.at[0, k], mate_out(k)))
        for k in range(1, outer)
    ]
    gb1 = [
        go(remote(sb.at[1, :, (i + k) % inner], rb1.at[k], ri_send.at[0, k], ri_recv.at[0, k], mate_in(k)))
        for k in range(1, inner)
    ]

    forwards = []

    def forward(place, send, recv):
        copy = remote(place, place, send, recv, partner)
        copy.start()
        forwards.append(copy)

    mine.wait()
    for k, copy in enumerate(a1, 1):
        copy.wait_recv()
    a2 = [
        go(remote(held_ref.at[o, :, :, rows(core, 0)], held_ref.at[o, :, :, rows(core, 0)],
                  go_send.at[1, k], go_recv.at[1, k], mate_out(k)))
        for k in range(1, outer)
    ]
    for k, copy in enumerate(b1, 1):
        copy.wait_recv()
    b2 = [
        go(remote(held_ref.at[:, i, :, rows(core, 1)], held_ref.at[:, i, :, rows(core, 1)],
                  gi_send.at[1, k], gi_recv.at[1, k], mate_in(k)))
        for k in range(1, inner)
    ]
    for k in range(1, inner):
        forward(held_ref.at[o, (i - k + inner) % inner, :, rows(core, 0)], fi_send.at[0, k], fi_recv.at[0, k])
    for k in range(1, outer):
        forward(held_ref.at[(o - k + outer) % outer, i, :, rows(core, 1)], fo_send.at[0, k], fo_recv.at[0, k])

    for copy in ga1:
        copy.wait_recv()

    def sum_a(s, _):
        ii, j = s // slots, s % slots
        total = sb[0, o, ii, j].astype(F32)
        for k in range(1, outer):
            total += ra1[k, ii, j].astype(F32)
        ta[ii, j] = total.astype(BF16)
        return 0

    lax.fori_loop(0, inner * slots, sum_a, 0)
    ga2 = [
        go(remote(ta.at[(i + k) % inner], ra2.at[k], ri_send.at[1, k], ri_recv.at[1, k], mate_in(k)))
        for k in range(1, inner)
    ]
    for copy in gb1:
        copy.wait_recv()

    def sum_b(s, _):
        oo, j = s // slots, s % slots
        total = sb[1, oo, i, j].astype(F32)
        for k in range(1, inner):
            total += rb1[k, oo, j].astype(F32)
        tb[oo, j] = total.astype(BF16)
        return 0

    lax.fori_loop(0, outer * slots, sum_b, 0)
    gb2 = [
        go(remote(tb.at[(o + k) % outer], rb2.at[k], ro_send.at[1, k], ro_recv.at[1, k], mate_out(k)))
        for k in range(1, outer)
    ]

    for k, copy in enumerate(a2, 1):
        copy.wait_recv()
        forward(held_ref.at[(o - k + outer) % outer, :, :, rows(core, 0)], fo_send.at[1, k], fo_recv.at[1, k])
    for k, copy in enumerate(b2, 1):
        copy.wait_recv()
        forward(held_ref.at[:, (i - k + inner) % inner, :, rows(core, 1)], fi_send.at[1, k], fi_recv.at[1, k])

    for copy in ga2 + gb2:
        copy.wait_recv()

    def last(j, _):
        total = ta[i, j].astype(F32)
        for k in range(1, inner):
            total += ra2[k, j].astype(F32)
        out_ref[j, rows(core, 0)] = total.astype(BF16)
        total = tb[o, j].astype(F32)
        for k in range(1, outer):
            total += rb2[k, j].astype(F32)
        out_ref[j, rows(core, 1)] = total.astype(BF16)
        return 0

    lax.fori_loop(0, slots, last, 0)
    place = out_ref.at[:, pl.ds(pl.multiple_of(core * half, half), half)]
    swap = remote(place, place, out_sems.at[0], out_sems.at[1], partner)
    swap.start()
    for copy in started:
        copy.wait_send()
    pair.wait_send()
    for copy in forwards:
        copy.wait()
    swap.wait()


def body(tokens, block_codes, scales, counts, cotangent):
    owners_total = lax.axis_size("fsdp")
    most_slots, tile = block_codes.shape[0], block_codes.shape[1]
    local_tokens, width = tokens.shape
    key_width = cotangent.shape[1]
    row_tiles, col_tiles = width // tile, key_width // tile
    block_count = row_tiles * col_tiles
    total_tokens = local_tokens * lax.axis_size("dp") * owners_total
    loss_scale = 1.0 / math.sqrt(total_tokens)
    inner = 4 if owners_total % 4 == 0 else 1
    outer = owners_total // inner
    half, q = tile // 2, tile // 4
    all_slots = owners_total * most_slots
    offsets, source_ids = block_index(counts, owners_total, block_count, most_slots)
    within = jnp.arange(most_slots, dtype=jnp.int32)
    wanted = jnp.clip(offsets[:, None] + within[None, :], 0, block_count - 1).reshape(all_slots)
    own_blocks = (block_codes.astype(F32) * scales[:, None, None]).astype(BF16)

    chunks = 8
    depth = width // chunks
    grads = pl.pallas_call(
        functools.partial(grad_kernel, loss_scale, tile),
        grid=(chunks,),
        in_specs=[
            pl.BlockSpec((local_tokens, depth), lambda g: (0, g)),
            pl.BlockSpec((local_tokens, key_width), lambda g: (0, 0)),
        ],
        out_specs=pl.BlockSpec((2, block_count // chunks, half, tile), lambda g: (0, g, 0, 0)),
        out_shape=jax.ShapeDtypeStruct((2, block_count, half, tile), BF16),
    )(tokens, cotangent)

    dma = pltpu.SemaphoreType.DMA
    vmem = pl.BlockSpec(memory_space=pltpu.VMEM)
    held, picked = pl.pallas_call(
        functools.partial(comm_kernel, outer, inner),
        in_specs=[pl.BlockSpec(memory_space=pltpu.SMEM), vmem, vmem],
        out_specs=[pl.BlockSpec(memory_space=pl.ANY), vmem],
        out_shape=[
            jax.ShapeDtypeStruct((outer, inner, most_slots, tile, tile), BF16),
            jax.ShapeDtypeStruct((most_slots, tile, tile), BF16),
        ],
        scratch_shapes=[
            pltpu.VMEM((block_count, half, tile), BF16),
            pltpu.VMEM((2, outer, inner, most_slots, q, tile), BF16),
            pltpu.VMEM((outer, inner, most_slots, q, tile), BF16),
            pltpu.VMEM((inner, outer, most_slots, q, tile), BF16),
            pltpu.VMEM((inner, most_slots, q, tile), BF16),
            pltpu.VMEM((outer, most_slots, q, tile), BF16),
            pltpu.VMEM((inner, most_slots, q, tile), BF16),
            pltpu.VMEM((outer, most_slots, q, tile), BF16),
            dma,
            dma((2,)),
            dma((2, inner)), dma((2, inner)), dma((2, outer)), dma((2, outer)),
            dma((2, inner)), dma((2, inner)), dma((2, outer)), dma((2, outer)),
            dma((2, inner)), dma((2, inner)), dma((2, outer)), dma((2, outer)),
            dma((2,)),
        ],
        compiler_params=pltpu.CompilerParams(
            collective_id=0, has_side_effects=True, vmem_limit_bytes=48 * 1024 * 1024
        ),
    )(wanted, own_blocks, grads)

    held = held.reshape(all_slots, tile, tile)
    projected, token_grad = pl.pallas_call(
        functools.partial(weight_kernel, tile, chunks),
        grid_spec=pltpu.PrefetchScalarGridSpec(
            num_scalar_prefetch=1,
            grid=(chunks,),
            in_specs=[
                pl.BlockSpec((local_tokens, depth), lambda g, ids: (0, g)),
                pl.BlockSpec((local_tokens, key_width), lambda g, ids: (0, 0)),
                pl.BlockSpec(memory_space=pl.ANY),
            ],
            out_specs=[
                pl.BlockSpec((local_tokens, key_width), lambda g, ids: (0, 0)),
                pl.BlockSpec((local_tokens, depth), lambda g, ids: (0, g)),
            ],
            scratch_shapes=[
                pltpu.VMEM((chunks, depth, key_width), BF16),
                pltpu.VMEM((local_tokens, key_width), F32),
                dma((chunks,)),
            ],
        ),
        out_shape=[
            jax.ShapeDtypeStruct((local_tokens, key_width), BF16),
            jax.ShapeDtypeStruct((local_tokens, width), BF16),
        ],
    )(source_ids, tokens, cotangent, held)

    is_mine = jnp.arange(owners_total, dtype=jnp.int32) == lax.axis_index("fsdp")
    my_count = jnp.sum(jnp.where(is_mine, counts, 0))
    block_grad = jnp.where((within < my_count)[:, None, None], picked, jnp.zeros_like(picked))
    return (projected, token_grad, block_grad)


def solution(mesh):
    return jax.shard_map(
        body,
        mesh=mesh,
        in_specs=(
            P(("dp", "fsdp"), None),
            P("fsdp", None, None),
            P("fsdp"),
            P(),
            P(("dp", "fsdp"), None),
        ),
        out_specs=(P(("dp", "fsdp"), None), P(("dp", "fsdp"), None), P("fsdp", None, None)),
        check_vma=False,
    )
```

```python
import functools
import math

import jax
import jax.numpy as jnp
from jax import lax
from jax.experimental import pallas as pl
from jax.experimental.pallas import tpu as pltpu
from jax.sharding import PartitionSpec as P

MESH = pl.DeviceIdType.MESH
F32 = jnp.float32
BF16 = jnp.bfloat16


def grad_kernel(scale, tile, tok_ref, cot_ref, out_ref):
    half = tile // 2
    part = lax.dot_general(
        tok_ref[...], cot_ref[...], (((0,), (0,)), ((), ())), preferred_element_type=F32
    )
    part = (part * scale).astype(BF16)
    rows, cols = part.shape[0] // tile, part.shape[1] // tile
    for r in range(rows):
        for c in range(cols):
            for h in range(2):
                top = r * tile + h * half
                out_ref[h, r * cols + c] = part[top : top + half, c * tile : (c + 1) * tile]


def weight_kernel(tile, chunks, owners, tok_ref, cot_ref, held_ref, proj_ref, tg_ref, w_ref, acc_ref, sems):
    step = pl.program_id(0)
    depth = w_ref.shape[1]
    cols = w_ref.shape[2] // tile
    rows = depth // tile

    @pl.when(step == 0)
    def _():
        def fetch(g, _):
            for r in range(rows):
                for c in range(cols):
                    b = (g * rows + r) * cols + c
                    pltpu.make_async_copy(
                        held_ref.at[b % owners, b // owners],
                        w_ref.at[g, pl.ds(r * tile, tile), pl.ds(c * tile, tile)],
                        sems.at[g],
                    ).start()
            return 0

        lax.fori_loop(0, chunks, fetch, 0)
        acc_ref[...] = jnp.zeros_like(acc_ref)

    pltpu.make_async_copy(w_ref.at[step], w_ref.at[step], sems.at[step]).wait()
    weight = w_ref[step]
    acc_ref[...] += jnp.dot(tok_ref[...], weight, preferred_element_type=F32)
    tg_ref[...] = lax.dot_general(
        cot_ref[...], weight, (((1,), (1,)), ((), ())), preferred_element_type=F32
    ).astype(BF16)

    @pl.when(step == chunks - 1)
    def _():
        proj_ref[...] = acc_ref[...].astype(BF16)


def comm_kernel(
    outer, inner, q0, counts_ref, scales_ref, codes_ref, g_ref, held_ref, out_ref,
    pair_buf, wsend, wrecv, stage, sb0, sb1, ra1, rb1, ta, tb, ra2, rb2, fin, gsend, grecv,
    local_sem, pair_sems, w_send, w_recv, x_send, x_recv, own_sems,
    gi_send, gi_recv, go_send, go_recv, fi_send, fi_recv, fo_send, fo_recv,
    ri_send, ri_recv, ro_send, ro_recv, out_sems,
):
    owners = outer * inner
    core = lax.axis_index("dp")
    other = 1 - core
    me = lax.axis_index("fsdp")
    o = me // inner
    i = me % inner
    slots, tile = codes_ref.shape[0], codes_ref.shape[1]
    even = stage.shape[0]
    half = tile // 2
    q1 = half - q0
    my_half = pl.ds(pl.multiple_of(core * half, half), half)
    parts = (pl.ds(0, q0), pl.ds(q0, q1))

    def rows(p):
        return pl.ds(pl.multiple_of(core * half + p * q0, q0), (q0, q1)[p])

    partner = (other, me)

    def mate_in(k):
        return (core, o * inner + (i + k) % inner)

    def mate_out(k):
        return (core, ((o + k) % outer) * inner + i)

    def mate(k):
        return (core, (me + k) % owners)

    def remote(src, dst, send, recv, device):
        return pltpu.make_async_remote_copy(
            src_ref=src, dst_ref=dst, send_sem=send, recv_sem=recv,
            device_id=device, device_id_type=MESH,
        )

    barrier = pltpu.get_barrier_semaphore()
    peers = [partner] + [mate(k) for k in range(1, owners)]
    for peer in peers:
        pl.semaphore_signal(barrier, inc=1, device_id=peer, device_id_type=MESH)
    pl.semaphore_wait(barrier, len(peers))

    started = []

    def go(copy):
        copy.start()
        started.append(copy)
        return copy

    pair = go(remote(g_ref.at[other], pair_buf, pair_sems.at[0], pair_sems.at[1], partner))

    offsets, ends, run, my_off, my_count = [], [], 0, 0, 0
    for d in range(owners):
        count = counts_ref[d]
        offsets.append(run)
        run = run + count
        ends.append(run)
        my_off = my_off + jnp.where(d < me, count, 0)
        my_count = my_count + jnp.where(d == me, count, 0)

    for k in range(owners):
        e = (me + k) % owners
        slot = jnp.minimum(lax.rem(e - my_off + even * owners, owners), slots - 1)
        block = (codes_ref[slot, my_half].astype(F32) * scales_ref[slot]).astype(BF16)
        if k == 0:
            wrecv[me] = block
        else:
            wsend[k] = block
    w_copies = [
        go(remote(wsend.at[k], wrecv.at[me], w_send.at[k], w_recv.at[k], mate(k)))
        for k in range(1, owners)
    ]

    pair.wait_recv()

    def build(s, _):
        oo, ii, m = s // (inner * even), (s // even) % inner, s % even
        b = m * owners + oo * inner + ii
        total = g_ref[core, b].astype(F32) + pair_buf[b].astype(F32)
        total = total.astype(BF16)
        sb0[oo, ii, m] = total[:q0]
        sb1[oo, ii, m] = total[q0:]
        return 0

    lax.fori_loop(0, owners * even, build, 0, unroll=4)

    ga1 = [
        go(remote(sb0.at[(o + k) % outer], ra1.at[k], ro_send.at[0, k], ro_recv.at[0, k], mate_out(k)))
        for k in range(1, outer)
    ]
    gb1 = [
        go(remote(sb1.at[:, (i + k) % inner], rb1.at[k], ri_send.at[0, k], ri_recv.at[0, k], mate_in(k)))
        for k in range(1, inner)
    ]

    for copy in w_copies:
        copy.wait_recv()
    for m in range(even):
        owner = 0
        for d in range(owners):
            owner = owner + jnp.where(ends[d] <= m * owners + me, 1, 0)
        stage[m] = wrecv[jnp.minimum(owner, owners - 1)]
    a1 = [
        go(remote(stage.at[:, parts[0]], held_ref.at[o, i, :, rows(0)],
                  gi_send.at[0, k], gi_recv.at[0, k], mate_in(k)))
        for k in range(1, inner)
    ]
    b1 = [
        go(remote(stage.at[:, parts[1]], held_ref.at[o, i, :, rows(1)],
                  go_send.at[0, k], go_recv.at[0, k], mate_out(k)))
        for k in range(1, outer)
    ]
    mine = pltpu.make_async_copy(stage, held_ref.at[o, i, :, my_half], local_sem)
    mine.start()
    forwards = []

    def forward(src, place, send, recv):
        copy = remote(src, place, send, recv, partner)
        copy.start()
        forwards.append(copy)

    forward(stage, held_ref.at[o, i, :, my_half], own_sems.at[0], own_sems.at[1])

    mine.wait()
    for copy in a1:
        copy.wait_recv()
    a2 = [
        go(remote(held_ref.at[o, :, :, rows(0)], held_ref.at[o, :, :, rows(0)],
                  go_send.at[1, k], go_recv.at[1, k], mate_out(k)))
        for k in range(1, outer)
    ]
    for copy in b1:
        copy.wait_recv()
    b2 = [
        go(remote(held_ref.at[:, i, :, rows(1)], held_ref.at[:, i, :, rows(1)],
                  gi_send.at[1, k], gi_recv.at[1, k], mate_in(k)))
        for k in range(1, inner)
    ]
    for k in range(1, inner):
        place = held_ref.at[o, (i - k + inner) % inner, :, rows(0)]
        forward(place, place, fi_send.at[0, k], fi_recv.at[0, k])
    for k in range(1, outer):
        place = held_ref.at[(o - k + outer) % outer, i, :, rows(1)]
        forward(place, place, fo_send.at[0, k], fo_recv.at[0, k])

    for copy in ga1:
        copy.wait_recv()

    def sum_a(s, _):
        ii, m = s // even, s % even
        total = sb0[o, ii, m].astype(F32)
        for k in range(1, outer):
            total += ra1[k, ii, m].astype(F32)
        ta[ii, m] = total.astype(BF16)
        return 0

    lax.fori_loop(0, inner * even, sum_a, 0)
    ga2 = [
        go(remote(ta.at[(i + k) % inner], ra2.at[k], ri_send.at[1, k], ri_recv.at[1, k], mate_in(k)))
        for k in range(1, inner)
    ]
    for copy in gb1:
        copy.wait_recv()

    def sum_b(s, _):
        oo, m = s // even, s % even
        total = sb1[oo, i, m].astype(F32)
        for k in range(1, inner):
            total += rb1[k, oo, m].astype(F32)
        tb[oo, m] = total.astype(BF16)
        return 0

    lax.fori_loop(0, outer * even, sum_b, 0)
    gb2 = [
        go(remote(tb.at[(o + k) % outer], rb2.at[k], ro_send.at[1, k], ro_recv.at[1, k], mate_out(k)))
        for k in range(1, outer)
    ]

    for copy in ga2 + gb2:
        copy.wait_recv()
    for m in range(even):
        total = ta[i, m].astype(F32)
        for k in range(1, inner):
            total += ra2[k, m].astype(F32)
        fin[m, parts[0]] = total.astype(BF16)
        total = tb[o, m].astype(F32)
        for k in range(1, outer):
            total += rb2[k, m].astype(F32)
        fin[m, parts[1]] = total.astype(BF16)
    for k in range(owners):
        d = (me + k) % owners
        start = 0
        for x in range(owners):
            start = start + jnp.where(x < d, counts_ref[x], 0)
        m = jnp.minimum(lax.div(start - me + owners - 1, owners), even - 1)
        if k == 0:
            grecv[me] = fin[m]
        else:
            gsend[k] = fin[m]
    x_copies = [
        go(remote(gsend.at[k], grecv.at[me], x_send.at[k], x_recv.at[k], mate(k)))
        for k in range(1, owners)
    ]

    for k, copy in enumerate(a2, 1):
        copy.wait_recv()
        place = held_ref.at[(o - k + outer) % outer, :, :, rows(0)]
        forward(place, place, fo_send.at[1, k], fo_recv.at[1, k])
    for k, copy in enumerate(b2, 1):
        copy.wait_recv()
        place = held_ref.at[:, (i - k + inner) % inner, :, rows(1)]
        forward(place, place, fi_send.at[1, k], fi_recv.at[1, k])

    for copy in x_copies:
        copy.wait_recv()
    for j in range(slots):
        used = jnp.where(j < my_count, 1.0, 0.0).astype(F32)
        block = grecv[lax.rem(my_off + j, owners)].astype(F32)
        out_ref[j, my_half] = (block * used).astype(BF16)
    place = out_ref.at[:, my_half]
    swap = remote(place, place, out_sems.at[0], out_sems.at[1], partner)
    swap.start()
    for copy in started:
        copy.wait_send()
    for copy in forwards:
        copy.wait()
    swap.wait()


def body(tokens, block_codes, scales, counts, cotangent):
    owners_total = lax.axis_size("fsdp")
    most_slots, tile = block_codes.shape[0], block_codes.shape[1]
    local_tokens, width = tokens.shape
    key_width = cotangent.shape[1]
    row_tiles, col_tiles = width // tile, key_width // tile
    block_count = row_tiles * col_tiles
    total_tokens = local_tokens * lax.axis_size("dp") * owners_total
    loss_scale = 1.0 / math.sqrt(total_tokens)
    inner = 4 if owners_total % 4 == 0 else 1
    outer = owners_total // inner
    even = block_count // owners_total
    half = tile // 2
    q0 = tile // 8
    q1 = half - q0
    assert even * owners_total == block_count and most_slots <= owners_total

    chunks = 8
    depth = width // chunks
    grads = pl.pallas_call(
        functools.partial(grad_kernel, loss_scale, tile),
        grid=(chunks,),
        in_specs=[
            pl.BlockSpec((local_tokens, depth), lambda g: (0, g)),
            pl.BlockSpec((local_tokens, key_width), lambda g: (0, 0)),
        ],
        out_specs=pl.BlockSpec((2, block_count // chunks, half, tile), lambda g: (0, g, 0, 0)),
        out_shape=jax.ShapeDtypeStruct((2, block_count, half, tile), BF16),
    )(tokens, cotangent)

    dma = pltpu.SemaphoreType.DMA
    vmem = pl.BlockSpec(memory_space=pltpu.VMEM)
    smem = pl.BlockSpec(memory_space=pltpu.SMEM)
    pairs_in, pairs_out = dma((2, inner)), dma((2, outer))
    held, block_grad = pl.pallas_call(
        functools.partial(comm_kernel, outer, inner, q0),
        in_specs=[smem, smem, vmem, vmem],
        out_specs=[pl.BlockSpec(memory_space=pl.ANY), vmem],
        out_shape=[
            jax.ShapeDtypeStruct((outer, inner, even, tile, tile), BF16),
            jax.ShapeDtypeStruct((most_slots, tile, tile), BF16),
        ],
        scratch_shapes=[
            pltpu.VMEM((block_count, half, tile), BF16),
            pltpu.VMEM((owners_total, half, tile), BF16),
            pltpu.VMEM((owners_total, half, tile), BF16),
            pltpu.VMEM((even, half, tile), BF16),
            pltpu.VMEM((outer, inner, even, q0, tile), BF16),
            pltpu.VMEM((outer, inner, even, q1, tile), BF16),
            pltpu.VMEM((outer, inner, even, q0, tile), BF16),
            pltpu.VMEM((inner, outer, even, q1, tile), BF16),
            pltpu.VMEM((inner, even, q0, tile), BF16),
            pltpu.VMEM((outer, even, q1, tile), BF16),
            pltpu.VMEM((inner, even, q0, tile), BF16),
            pltpu.VMEM((outer, even, q1, tile), BF16),
            pltpu.VMEM((even, half, tile), BF16),
            pltpu.VMEM((owners_total, half, tile), BF16),
            pltpu.VMEM((owners_total, half, tile), BF16),
            dma,
            dma((2,)),
            dma((owners_total,)), dma((owners_total,)), dma((owners_total,)), dma((owners_total,)),
            dma((2,)),
            pairs_in, pairs_in, pairs_out, pairs_out,
            pairs_in, pairs_in, pairs_out, pairs_out,
            pairs_in, pairs_in, pairs_out, pairs_out,
            dma((2,)),
        ],
        compiler_params=pltpu.CompilerParams(
            collective_id=0, has_side_effects=True, vmem_limit_bytes=48 * 1024 * 1024
        ),
    )(counts, scales, block_codes, grads)

    held = held.reshape(owners_total, even, tile, tile)
    projected, token_grad = pl.pallas_call(
        functools.partial(weight_kernel, tile, chunks, owners_total),
        grid_spec=pltpu.PrefetchScalarGridSpec(
            num_scalar_prefetch=0,
            grid=(chunks,),
            in_specs=[
                pl.BlockSpec((local_tokens, depth), lambda g: (0, g)),
                pl.BlockSpec((local_tokens, key_width), lambda g: (0, 0)),
                pl.BlockSpec(memory_space=pl.ANY),
            ],
            out_specs=[
                pl.BlockSpec((local_tokens, key_width), lambda g: (0, 0)),
                pl.BlockSpec((local_tokens, depth), lambda g: (0, g)),
            ],
            scratch_shapes=[
                pltpu.VMEM((chunks, depth, key_width), BF16),
                pltpu.VMEM((local_tokens, key_width), F32),
                dma((chunks,)),
            ],
        ),
        out_shape=[
            jax.ShapeDtypeStruct((local_tokens, key_width), BF16),
            jax.ShapeDtypeStruct((local_tokens, width), BF16),
        ],
    )(tokens, cotangent, held)

    return (projected, token_grad, block_grad)


def solution(mesh):
    return jax.shard_map(
        body,
        mesh=mesh,
        in_specs=(
            P(("dp", "fsdp"), None),
            P("fsdp", None, None),
            P("fsdp"),
            P(),
            P(("dp", "fsdp"), None),
        ),
        out_specs=(P(("dp", "fsdp"), None), P(("dp", "fsdp"), None), P("fsdp", None, None)),
        check_vma=False,
    )
```

```python
import functools
import math

import jax
import jax.numpy as jnp
from jax import lax
from jax.experimental import pallas as pl
from jax.experimental.pallas import tpu as pltpu
from jax.sharding import PartitionSpec as P

MESH = pl.DeviceIdType.MESH
F32 = jnp.float32
BF16 = jnp.bfloat16


def comm_kernel(
    outer, inner, q0, scale, counts_ref, scales_ref, codes_ref, tok_ref, cot_ref, proj_ref, tg_ref, out_ref,
    g_ref, held_ref, w_ref, acc_ref, pair_buf, wsend, wrecv, stage, sb0, sb1, ra1, rb1, ta, tb, ra2, rb2, fin, gsend, grecv,
    pair_sems, w_send, w_recv, x_send, x_recv, own_sems,
    gi_send, gi_recv, go_send, go_recv, fi_send, fi_recv, fo_send, fo_recv,
    ri_send, ri_recv, ro_send, ro_recv, out_sems,
):
    owners = outer * inner
    core = lax.axis_index("dp")
    other = 1 - core
    me = lax.axis_index("fsdp")
    o = me // inner
    i = me % inner
    slots, tile = codes_ref.shape[0], codes_ref.shape[1]
    even = stage.shape[0]
    half = tile // 2
    q1 = half - q0
    my_half = pl.ds(pl.multiple_of(core * half, half), half)
    parts = (pl.ds(0, q0), pl.ds(q0, q1))

    def rows(p):
        return pl.ds(pl.multiple_of(core * half + p * q0, q0), (q0, q1)[p])

    partner = (other, me)

    def mate_in(k):
        return (core, o * inner + (i + k) % inner)

    def mate_out(k):
        return (core, ((o + k) % outer) * inner + i)

    def mate(k):
        return (core, (me + k) % owners)

    def remote(src, dst, send, recv, device):
        return pltpu.make_async_remote_copy(
            src_ref=src, dst_ref=dst, send_sem=send, recv_sem=recv,
            device_id=device, device_id_type=MESH,
        )

    barrier = pltpu.get_barrier_semaphore()
    peers = [partner] + [mate(k) for k in range(1, owners)]
    for peer in peers:
        pl.semaphore_signal(barrier, inc=1, device_id=peer, device_id_type=MESH)
    pl.semaphore_wait(barrier, len(peers))

    started = []

    def go(copy):
        copy.start()
        started.append(copy)
        return copy

    offsets, ends, run, my_off, my_count = [], [], 0, 0, 0
    for d in range(owners):
        count = counts_ref[d]
        offsets.append(run)
        run = run + count
        ends.append(run)
        my_off = my_off + jnp.where(d < me, count, 0)
        my_count = my_count + jnp.where(d == me, count, 0)

    for k in range(owners):
        e = (me + k) % owners
        slot = jnp.minimum(lax.rem(e - my_off + even * owners, owners), slots - 1)
        block = (codes_ref[slot, my_half].astype(F32) * scales_ref[slot]).astype(BF16)
        if k == 0:
            wrecv[me] = block
        else:
            wsend[k] = block
    w_copies = [
        go(remote(wsend.at[k], wrecv.at[me], w_send.at[k], w_recv.at[k], mate(k)))
        for k in range(1, owners)
    ]

    depth = w_ref.shape[0]
    chunks = tok_ref.shape[1] // depth
    row_tiles, col_tiles = depth // tile, cot_ref.shape[1] // tile

    def terms(g, _):
        columns = pl.ds(pl.multiple_of(g * depth, depth), depth)
        part = lax.dot_general(
            tok_ref[:, columns], cot_ref[...], (((0,), (0,)), ((), ())), preferred_element_type=F32
        )
        part = (part * scale).astype(BF16)
        for r in range(row_tiles):
            for c in range(col_tiles):
                for h in range(2):
                    top = r * tile + h * half
                    g_ref[h, (g * row_tiles + r) * col_tiles + c] = part[
                        top : top + half, c * tile : (c + 1) * tile
                    ]
        return 0

    lax.fori_loop(0, chunks, terms, 0)
    pair = go(remote(g_ref.at[other], pair_buf, pair_sems.at[0], pair_sems.at[1], partner))

    for copy in w_copies:
        copy.wait_recv()
    for m in range(even):
        owner = 0
        for d in range(owners):
            owner = owner + jnp.where(ends[d] <= m * owners + me, 1, 0)
        block = wrecv[jnp.minimum(owner, owners - 1)]
        stage[m] = block
        held_ref[o, i, m, my_half] = block
    a1 = [
        go(remote(stage.at[:, parts[0]], held_ref.at[o, i, :, rows(0)],
                  gi_send.at[0, k], gi_recv.at[0, k], mate_in(k)))
        for k in range(1, inner)
    ]
    b1 = [
        go(remote(stage.at[:, parts[1]], held_ref.at[o, i, :, rows(1)],
                  go_send.at[0, k], go_recv.at[0, k], mate_out(k)))
        for k in range(1, outer)
    ]
    forwards = []

    def forward(src, place, send, recv):
        copy = remote(src, place, send, recv, partner)
        copy.start()
        forwards.append(copy)

    forward(stage, held_ref.at[o, i, :, my_half], own_sems.at[0], own_sems.at[1])

    pair.wait_recv()

    def build(s, _):
        oo, ii, m = s // (inner * even), (s // even) % inner, s % even
        b = m * owners + oo * inner + ii
        total = g_ref[core, b].astype(F32) + pair_buf[b].astype(F32)
        total = total.astype(BF16)
        sb0[oo, ii, m] = total[:q0]
        sb1[oo, ii, m] = total[q0:]
        return 0

    lax.fori_loop(0, owners * even, build, 0, unroll=4)

    ga1 = [
        go(remote(sb0.at[(o + k) % outer], ra1.at[k], ro_send.at[0, k], ro_recv.at[0, k], mate_out(k)))
        for k in range(1, outer)
    ]
    gb1 = [
        go(remote(sb1.at[:, (i + k) % inner], rb1.at[k], ri_send.at[0, k], ri_recv.at[0, k], mate_in(k)))
        for k in range(1, inner)
    ]

    for copy in a1:
        copy.wait_recv()
    a2 = [
        go(remote(held_ref.at[o, :, :, rows(0)], held_ref.at[o, :, :, rows(0)],
                  go_send.at[1, k], go_recv.at[1, k], mate_out(k)))
        for k in range(1, outer)
    ]
    for copy in b1:
        copy.wait_recv()
    b2 = [
        go(remote(held_ref.at[:, i, :, rows(1)], held_ref.at[:, i, :, rows(1)],
                  gi_send.at[1, k], gi_recv.at[1, k], mate_in(k)))
        for k in range(1, inner)
    ]
    for k in range(1, inner):
        place = held_ref.at[o, (i - k + inner) % inner, :, rows(0)]
        forward(place, place, fi_send.at[0, k], fi_recv.at[0, k])
    for k in range(1, outer):
        place = held_ref.at[(o - k + outer) % outer, i, :, rows(1)]
        forward(place, place, fo_send.at[0, k], fo_recv.at[0, k])

    for copy in ga1:
        copy.wait_recv()

    def sum_a(s, _):
        ii, m = s // even, s % even
        total = sb0[o, ii, m].astype(F32)
        for k in range(1, outer):
            total += ra1[k, ii, m].astype(F32)
        ta[ii, m] = total.astype(BF16)
        return 0

    lax.fori_loop(0, inner * even, sum_a, 0)
    ga2 = [
        go(remote(ta.at[(i + k) % inner], ra2.at[k], ri_send.at[1, k], ri_recv.at[1, k], mate_in(k)))
        for k in range(1, inner)
    ]
    for copy in gb1:
        copy.wait_recv()

    def sum_b(s, _):
        oo, m = s // even, s % even
        total = sb1[oo, i, m].astype(F32)
        for k in range(1, inner):
            total += rb1[k, oo, m].astype(F32)
        tb[oo, m] = total.astype(BF16)
        return 0

    lax.fori_loop(0, outer * even, sum_b, 0)
    gb2 = [
        go(remote(tb.at[(o + k) % outer], rb2.at[k], ro_send.at[1, k], ro_recv.at[1, k], mate_out(k)))
        for k in range(1, outer)
    ]

    for k, copy in enumerate(a2, 1):
        copy.wait_recv()
        place = held_ref.at[(o - k + outer) % outer, :, :, rows(0)]
        forward(place, place, fo_send.at[1, k], fo_recv.at[1, k])
    for k, copy in enumerate(b2, 1):
        copy.wait_recv()
        place = held_ref.at[:, (i - k + inner) % inner, :, rows(1)]
        forward(place, place, fi_send.at[1, k], fi_recv.at[1, k])

    for copy in ga2 + gb2:
        copy.wait_recv()
    for m in range(even):
        total = ta[i, m].astype(F32)
        for k in range(1, inner):
            total += ra2[k, m].astype(F32)
        fin[m, parts[0]] = total.astype(BF16)
        total = tb[o, m].astype(F32)
        for k in range(1, outer):
            total += rb2[k, m].astype(F32)
        fin[m, parts[1]] = total.astype(BF16)
    for k in range(owners):
        d = (me + k) % owners
        start = 0
        for x in range(owners):
            start = start + jnp.where(x < d, counts_ref[x], 0)
        m = jnp.minimum(lax.div(start - me + owners - 1, owners), even - 1)
        if k == 0:
            grecv[me] = fin[m]
        else:
            gsend[k] = fin[m]
    x_copies = [
        go(remote(gsend.at[k], grecv.at[me], x_send.at[k], x_recv.at[k], mate(k)))
        for k in range(1, owners)
    ]

    for copy in forwards:
        copy.wait_recv()
    acc_ref[...] = jnp.zeros_like(acc_ref)

    def products(g, _):
        columns = pl.ds(pl.multiple_of(g * depth, depth), depth)
        for r in range(row_tiles):
            for c in range(col_tiles):
                b = (g * row_tiles + r) * col_tiles + c
                e, m = b % owners, b // owners
                w_ref[r * tile : (r + 1) * tile, c * tile : (c + 1) * tile] = held_ref[e // inner, e % inner, m]
        weight = w_ref[...]
        acc_ref[...] += jnp.dot(tok_ref[:, columns], weight, preferred_element_type=F32)
        tg_ref[:, columns] = lax.dot_general(
            cot_ref[...], weight, (((1,), (1,)), ((), ())), preferred_element_type=F32
        ).astype(BF16)
        return 0

    lax.fori_loop(0, chunks, products, 0)
    proj_ref[...] = acc_ref[...].astype(BF16)

    for copy in x_copies:
        copy.wait_recv()
    for j in range(slots):
        used = jnp.where(j < my_count, 1.0, 0.0).astype(F32)
        block = grecv[lax.rem(my_off + j, owners)].astype(F32)
        out_ref[j, my_half] = (block * used).astype(BF16)
    place = out_ref.at[:, my_half]
    swap = remote(place, place, out_sems.at[0], out_sems.at[1], partner)
    swap.start()
    for copy in started:
        copy.wait_send()
    for copy in forwards:
        copy.wait_send()
    swap.wait()


def body(tokens, block_codes, scales, counts, cotangent):
    owners_total = lax.axis_size("fsdp")
    most_slots, tile = block_codes.shape[0], block_codes.shape[1]
    local_tokens, width = tokens.shape
    key_width = cotangent.shape[1]
    row_tiles, col_tiles = width // tile, key_width // tile
    block_count = row_tiles * col_tiles
    total_tokens = local_tokens * lax.axis_size("dp") * owners_total
    loss_scale = 1.0 / math.sqrt(total_tokens)
    inner = 4 if owners_total % 4 == 0 else 1
    outer = owners_total // inner
    even = block_count // owners_total
    half = tile // 2
    q0 = tile // 8
    q1 = half - q0
    assert even * owners_total == block_count and most_slots <= owners_total

    chunks = 8
    depth = width // chunks
    dma = pltpu.SemaphoreType.DMA
    vmem = pl.BlockSpec(memory_space=pltpu.VMEM)
    smem = pl.BlockSpec(memory_space=pltpu.SMEM)
    pairs_in, pairs_out = dma((2, inner)), dma((2, outer))
    return tuple(pl.pallas_call(
        functools.partial(comm_kernel, outer, inner, q0, loss_scale),
        in_specs=[smem, smem, vmem, vmem, vmem],
        out_specs=[vmem, vmem, vmem],
        out_shape=[
            jax.ShapeDtypeStruct((local_tokens, key_width), BF16),
            jax.ShapeDtypeStruct((local_tokens, width), BF16),
            jax.ShapeDtypeStruct((most_slots, tile, tile), BF16),
        ],
        scratch_shapes=[
            pltpu.VMEM((2, block_count, half, tile), BF16),
            pltpu.VMEM((outer, inner, even, tile, tile), BF16),
            pltpu.VMEM((depth, key_width), BF16),
            pltpu.VMEM((local_tokens, key_width), F32),
            pltpu.VMEM((block_count, half, tile), BF16),
            pltpu.VMEM((owners_total, half, tile), BF16),
            pltpu.VMEM((owners_total, half, tile), BF16),
            pltpu.VMEM((even, half, tile), BF16),
            pltpu.VMEM((outer, inner, even, q0, tile), BF16),
            pltpu.VMEM((outer, inner, even, q1, tile), BF16),
            pltpu.VMEM((outer, inner, even, q0, tile), BF16),
            pltpu.VMEM((inner, outer, even, q1, tile), BF16),
            pltpu.VMEM((inner, even, q0, tile), BF16),
            pltpu.VMEM((outer, even, q1, tile), BF16),
            pltpu.VMEM((inner, even, q0, tile), BF16),
            pltpu.VMEM((outer, even, q1, tile), BF16),
            pltpu.VMEM((even, half, tile), BF16),
            pltpu.VMEM((owners_total, half, tile), BF16),
            pltpu.VMEM((owners_total, half, tile), BF16),
            dma((2,)),
            dma((owners_total,)), dma((owners_total,)), dma((owners_total,)), dma((owners_total,)),
            dma((2,)),
            pairs_in, pairs_in, pairs_out, pairs_out,
            pairs_in, pairs_in, pairs_out, pairs_out,
            pairs_in, pairs_in, pairs_out, pairs_out,
            dma((2,)),
        ],
        compiler_params=pltpu.CompilerParams(
            collective_id=0, has_side_effects=True, vmem_limit_bytes=48 * 1024 * 1024
        ),
    )(counts, scales, block_codes, tokens, cotangent))


def solution(mesh):
    return jax.shard_map(
        body,
        mesh=mesh,
        in_specs=(
            P(("dp", "fsdp"), None),
            P("fsdp", None, None),
            P("fsdp"),
            P(),
            P(("dp", "fsdp"), None),
        ),
        out_specs=(P(("dp", "fsdp"), None), P(("dp", "fsdp"), None), P("fsdp", None, None)),
        check_vma=False,
    )
```
